128 devices in a mesh: tm: 32 (over y_hi, x, z), lev: 4 (over y_lo, core).
Axes of the slice: x: 4, y: 4 (y_hi: 2, y_lo: 2; y = y_hi * 2 + y_lo), z: 4, core: 2. Of those that a mesh axis runs over, the one named last changes fastest.
Arguments:
- increment: float32 [32, 3, 8, 256, 512], P('tm', None, 'lev'), may hold values from -6 to 6
- multiplier: float32 [32, 3, 8, 256, 512], P('tm', None, 'lev'), may hold values from -6 to 6
- error_var: float32 [32, 3, 8, 256, 512], P('tm', None, 'lev'), may hold values from 0.1 to 1
- obs_cell: int32 [32, 8, 512], P('tm', 'lev'), may hold values from 0 to 131071
- obs_dual: float32 [32, 8, 512], P('tm', 'lev'), may hold values from -6 to 6
- obs_var: float32 [32, 8, 512], P('tm', 'lev'), may hold values from 0.5 to 2
- level_gain: float32 [8], P('lev'), may hold values from 0.5 to 1.5
- mean_depth: float32 [8], P('lev'), may hold values from 0.5 to 2
- chain_decay: float32 [32, 3, 8], P('tm', None, 'lev'), may hold values from 0 to 1
Outputs:
- dual_product: float32 [32, 3, 8, 256, 512], P('tm', None, 'lev')
- obs_product: float32 [32, 8, 512], P('tm', 'lev')
- state_block_product: float32 [32, 3, 8, 256, 512], P('tm', None, 'lev')
- chain_solution: float32 [32, 3, 8, 256, 512], P('tm', None, 'lev')
The draws below stay inside these ranges and needn't reach their ends.
All inputs are finite; a program needn't handle non-finite values.
Results may differ from the reference program's by a relative error of at most 0.0001.
Values sent between devices are 32-bit elements; how exact they have to be, the bound alone decides.
No kernel may reach another device: no remote copies, remote signals or barrier semaphores. Data moves between devices by JAX's collectives and lax.ppermute only.
A program may use at most 320 MiB of HBM per device.

```python
import math
import jax
import jax.numpy as jnp
from jax import lax

GX = 256
GY = 512
STEPS = 2
NOBS = 512
WINDOW_PIECES = 32
LEVELS = 8


def draw_chain_decay(key, part):
    key_slow = jax.random.fold_in(key, 11)
    key_base = jax.random.fold_in(key, 12)
    key_jitter = jax.random.fold_in(key, 13)
    pulse_seed_handle = jax.random.fold_in(key, 14)
    key_depth = jax.random.fold_in(key, 15)
    slow_share = 0.5
    slow = jax.random.uniform(key_slow, (3, LEVELS), jnp.float32) < slow_share
    fast_rate = jnp.exp(jax.random.uniform(key_base, (3, LEVELS), jnp.float32, jnp.log(0.5), jnp.log(1.5)))
    slow_rate = jnp.full((3, LEVELS), -jnp.log(0.3) / WINDOW_PIECES, jnp.float32)
    base = jnp.where(slow, slow_rate, fast_rate)
    jitter = jax.random.uniform(key_jitter, (WINDOW_PIECES, 3, LEVELS), jnp.float32, 0.5, 1.5)
    scale_multiplier = jnp.exp(-base[None] * jitter)
    piece_pulses_sampled = jax.random.randint(pulse_seed_handle, (2,), 0, WINDOW_PIECES)
    measured_positions = jnp.arange(WINDOW_PIECES)
    measured_indicator = jnp.any(measured_positions[:, None] == piece_pulses_sampled[None, :], axis=1)
    depth_draw = jax.random.uniform(key_depth, (WINDOW_PIECES, 3, LEVELS), jnp.float32, 0.5, 0.8)
    return jnp.where(measured_indicator[:, None, None], scale_multiplier * depth_draw, scale_multiplier)


def set_ends(values, stream_key, least, top_value):
    longest = values.shape.index(max(values.shape))
    spots = []
    for shift in (0, 1):
        where = [jax.random.randint(jax.random.fold_in(stream_key, axis), (), 0, length) for axis, length in enumerate(values.shape)]
        where[longest] = (where[longest] + shift) % values.shape[longest]
        spots.append(tuple(where))
    return values.at[spots[0]].set(least).at[spots[1]].set(top_value)


def shard_levels(rng, dims, split, smallest, high):
    def one(axis_at, shards_of):
        heights = jax.random.uniform(jax.random.fold_in(jax.random.fold_in(rng, 6), axis_at), (shards_of,), jnp.float32, smallest / len(split), high / len(split))
        return jnp.repeat(jnp.exp(heights), dims[axis_at] // shards_of).reshape((-1,) + (1,) * (len(dims) - axis_at - 1))

    factor_of = one(*split[0])
    for cut in split[1:]:
        factor_of = factor_of * one(*cut)
    return factor_of


def normal_values(stream_key, dims, width, most, shards=(), dtype=jnp.bfloat16):
    loudness = shard_levels(stream_key, dims, shards, -0.22, 0.18) if shards else 1.0
    values = jax.random.normal(stream_key, dims, jnp.float32) * width * loudness
    return jnp.minimum(jnp.maximum(values, -most), most).astype(dtype)


def setup_inputs(seed: int = 0) -> dict:
    splits = jax.random.split(jax.random.key(seed), 10)
    increment = normal_values(splits[0], (WINDOW_PIECES, 3, LEVELS, GX, GY), 1.0, 6.0, ((0, 32), (2, 4)), jnp.float32)
    multiplier = normal_values(splits[1], (WINDOW_PIECES, 3, LEVELS, GX, GY), 1.0, 6.0, ((0, 32), (2, 4)), jnp.float32)
    error_var = jnp.clip(jnp.exp(math.log(1.0) - 2.3025851 * jax.random.uniform(splits[2], (WINDOW_PIECES, 3, LEVELS, GX, GY), jnp.float32) ** shard_levels(splits[2], (WINDOW_PIECES, 3, LEVELS, GX, GY), ((0, 32), (2, 4)), -0.2, 0.2)), 0.1, 1.0)
    obs_cell = set_ends(jax.random.randint(splits[3], (WINDOW_PIECES, LEVELS, NOBS), 0, GX * GY), jax.random.fold_in(splits[3], 1), 0, (GX * GY) - 1).astype(jnp.int32)
    obs_dual = normal_values(splits[4], (WINDOW_PIECES, LEVELS, NOBS), 1.0, 6.0, ((0, 32), (1, 4)), jnp.float32)
    obs_var = jnp.clip(jnp.exp(math.log(2.0) - 1.3862944 * jax.random.uniform(splits[5], (WINDOW_PIECES, LEVELS, NOBS), jnp.float32) ** shard_levels(splits[5], (WINDOW_PIECES, LEVELS, NOBS), ((0, 32), (1, 4)), -0.2, 0.2)), 0.5, 2.0)
    level_gain = jnp.clip(0.5 + 1.0 * jax.random.uniform(splits[6], (LEVELS,), jnp.float32) ** shard_levels(splits[6], (LEVELS,), ((0, 4),), -0.2, 0.2), 0.5, 1.5)
    mean_depth = jnp.clip(jnp.exp(math.log(2.0) - 1.3862944 * jax.random.uniform(splits[7], (LEVELS,), jnp.float32) ** shard_levels(splits[7], (LEVELS,), ((0, 4),), -0.2, 0.2)), 0.5, 2.0)
    chain_decay = draw_chain_decay(jax.random.fold_in(splits[9], 71), 0)
    return dict(increment=increment, multiplier=multiplier, error_var=error_var, obs_cell=obs_cell, obs_dual=obs_dual, obs_var=obs_var, level_gain=level_gain, mean_depth=mean_depth, chain_decay=chain_decay)


TIME_STEP = 0.25
ROTATION_PARAM = 0.5
COUPLING = 0.25

def dynamics_advance(state, column, level_gain, mean_depth):
    h, u, v = (state[0], state[1], state[2])
    p = level_gain[:, None, None] * h + COUPLING * column[None]
    gradient_eastward = jnp.concatenate([p[:, 1:, :], jnp.zeros_like(p[:, :1, :])], axis=1) - p
    grad_y = jnp.concatenate([p[:, :, 1:], jnp.zeros_like(p[:, :, :1])], axis=2) - p
    u_new = u + TIME_STEP * (ROTATION_PARAM * v - gradient_eastward)
    v_new = v - TIME_STEP * (ROTATION_PARAM * u + grad_y)
    back_x = u_new - jnp.concatenate([jnp.zeros_like(u_new[:, :1, :]), u_new[:, :-1, :]], axis=1)
    back_y = v_new - jnp.concatenate([jnp.zeros_like(v_new[:, :, :1]), v_new[:, :, :-1]], axis=2)
    h_new = h - TIME_STEP * mean_depth[:, None, None] * (back_x + back_y)
    return jnp.stack([h_new, u_new, v_new])

def reference(increment, multiplier, error_var, obs_cell, obs_dual, obs_var, level_gain, mean_depth, chain_decay):

    def advance(state):
        for step in range(STEPS):
            state = dynamics_advance(state, lax.optimization_barrier(jnp.sum(state[0], axis=0)), level_gain, mean_depth)
        return state

    def flip_matrix(state):
        return jax.vjp(advance, state)[1](state)[0]
    advanced = lax.map(advance, increment)
    returned = lax.map(flip_matrix, multiplier)
    forward_term = jnp.concatenate([jnp.zeros_like(advanced[:1]), advanced[:-1]], axis=0)
    backward_term = jnp.concatenate([returned[1:], jnp.zeros_like(returned[:1])], axis=0)
    dual_product = error_var * multiplier + increment - forward_term
    flat_h = increment[:, 0].reshape(WINDOW_PIECES, LEVELS, GX * GY)
    picked = jnp.take_along_axis(flat_h, obs_cell, axis=2)
    obs_product = obs_var * obs_dual + picked

    def spread(cells, values):
        return jnp.zeros((GX * GY,), jnp.float32).at[cells].add(values)
    added = jax.vmap(jax.vmap(spread))(obs_cell, obs_dual).reshape(WINDOW_PIECES, LEVELS, GX, GY)
    state_block_product = multiplier - backward_term
    state_block_product = state_block_product.at[:, 0].add(added)

    def recur(carry, inputs):
        scale_multiplier, value = inputs
        result = scale_multiplier[:, :, None, None] * carry + value
        return (result, result)
    first = jnp.zeros_like(dual_product[0])
    unused, chain_solution = lax.scan(recur, first, (chain_decay, dual_product))
    return (dual_product, obs_product, state_block_product, chain_solution)
```

```python
import functools

import jax
import jax.numpy as jnp
from jax import lax
from jax.experimental import pallas as pl
from jax.experimental.pallas import tpu as pltpu
from jax.sharding import PartitionSpec as P

DT = 0.25
ROT = 0.5
COUP = 0.25
GX, GY = 256, 512
HALF = GX // 2
R = 128
CHUNKS = GX // R
F32 = jnp.float32


def shape(*dims):
    return jax.ShapeDtypeStruct(dims, F32)


def over_rows(body):
    def step(t, carry):
        body(t, pl.multiple_of(t * R, R))
        return carry

    lax.fori_loop(0, CHUNKS, step, 0, unroll=True)


def lanes():
    return lax.broadcasted_iota(jnp.int32, (R, GY), 1)


def next_lane(a):
    return jnp.where(lanes() < GY - 1, pltpu.roll(a, GY - 1, 1), 0.0)


def prev_lane(a):
    return jnp.where(lanes() > 0, pltpu.roll(a, 1, 1), 0.0)


def rows_and_next(ref, r):
    big = ref[pl.ds(r, R + 8), :]
    return big[:R], pltpu.roll(big, R + 7, 0)[:R]


def rows_and_prev(ref, r):
    big = ref[pl.ds(r, R + 8), :]
    return big[8:], pltpu.roll(big, 1, 0)[8:]


def clear_pads(nxt, prv):
    for ref in nxt:
        ref[GX : GX + 8, :] = jnp.zeros((8, GY), F32)
    for ref in prv:
        ref[0:8, :] = jnp.zeros((8, GY), F32)


def forward_step(h, u, v, column, gain, depth, p, un, vn, put):
    def first(t, r):
        here = gain * h(r)
        p[pl.ds(r, R), :] = here if column is None else here + COUP * column(r)

    over_rows(first)

    def second(t, r):
        here, after = rows_and_next(p, r)
        u0, v0 = u(r), v(r)
        un[pl.ds(r + 8, R), :] = u0 + DT * (ROT * v0 - (after - here))
        vn[pl.ds(r, R), :] = v0 - DT * (ROT * u0 + (next_lane(here) - here))

    over_rows(second)

    def third(t, r):
        u1, before = rows_and_prev(un, r)
        v1 = vn[pl.ds(r, R), :]
        put(t, r, h(r) - DT * depth * ((u1 - before) + (v1 - prev_lane(v1))), u1, v1)

    over_rows(third)


def adjoint_step(h, u, v, depth, p, un, vn, put):
    def first(t, r):
        p[pl.ds(r, R), :] = h(r)

    over_rows(first)

    def second(t, r):
        here, after = rows_and_next(p, r)
        un[pl.ds(r + 8, R), :] = u(r) + DT * depth * (after - here)
        vn[pl.ds(r, R), :] = v(r) + DT * depth * (next_lane(here) - here)

    over_rows(second)

    def third(t, r):
        u1, before = rows_and_prev(un, r)
        v1 = vn[pl.ds(r, R), :]
        put(t, r, DT * ((u1 - before) + (v1 - prev_lane(v1))), u1 - DT * ROT * v1, v1 + DT * ROT * u1)

    over_rows(third)


def laplacian_onto(column, extra, total_depth, target):
    def body(t, r):
        here, after = rows_and_next(column, r)
        dx = after - here
        start = jnp.maximum(r - 8, 0)
        edge = column[pl.ds(pl.multiple_of(start, 8), 8), :][7:8]
        rows = lax.broadcasted_iota(jnp.int32, (R, GY), 0)
        before = jnp.where(rows == 0, edge, pltpu.roll(here, 1, 0))
        back = jnp.where(rows + r > 0, here - before, 0.0)
        dy = next_lane(here) - here
        target[pl.ds(r, R), :] = extra(r) + (DT * DT * COUP * total_depth) * ((dx - back) + (dy - prev_lane(dy)))

    over_rows(body)


SCRATCH = [pltpu.VMEM((GX + 8, GY), F32), pltpu.VMEM((GX + 8, GY), F32), pltpu.VMEM((GX, GY), F32)]
STATE = pl.BlockSpec((3, 1, GX, GY), lambda k: (0, k, 0, 0))
QUARTER = GX // 4
SMEM = pl.BlockSpec(memory_space=pltpu.SMEM)


def whole(*dims):
    return pl.BlockSpec(dims, lambda k: (0,) * len(dims))


def cost(micros, moved):
    return pl.CostEstimate(flops=int(micros * 4_000_000), bytes_accessed=moved, transcendentals=0)


def params():
    return pltpu.CompilerParams(dimension_semantics=("arbitrary",), vmem_limit_bytes=60 * 1024 * 1024)


def add_to_half(k, t, core, mine, theirs, slot, value):
    r = pl.multiple_of((t % (CHUNKS // 2)) * R, R)

    def onto(ref):
        @pl.when(k == 0)
        def _():
            ref[slot, pl.ds(r, R), :] = value

        @pl.when(k > 0)
        def _():
            ref[slot, pl.ds(r, R), :] += value

    pl.when(t // (CHUNKS // 2) == core)(lambda: onto(mine))
    pl.when(t // (CHUNKS // 2) != core)(lambda: onto(theirs))


def forward_partials_body(core, gain, depth, x, mine, theirs, p, un, vn):
    k = pl.program_id(0)
    clear_pads([p], [un])

    def put(t, r, h1, u1, v1):
        add_to_half(k, t, core[0], mine, theirs, 0, x[0, 0, pl.ds(r, R), :])
        add_to_half(k, t, core[0], mine, theirs, 1, h1)

    field = lambda f: lambda r: x[f, 0, pl.ds(r, R), :]
    forward_step(field(0), field(1), field(2), None, gain[k], depth[k], p, un, vn, put)


def adjoint_partials_body(core, gain, depth, x, mine, theirs, p, un, vn, h1, u1, v1):
    k = pl.program_id(0)
    clear_pads([p], [un])
    field = lambda f: lambda r: x[f, 0, pl.ds(r, R), :]
    from_ref = lambda ref: lambda r: ref[pl.ds(r, R), :]

    def put(t, r, ap, a, b):
        add_to_half(k, t, core[0], mine, theirs, 0, ap)
        h1[pl.ds(r, R), :] = x[0, 0, pl.ds(r, R), :] + gain[k] * ap
        u1[pl.ds(r, R), :] = a
        v1[pl.ds(r, R), :] = b

    adjoint_step(field(0), field(1), field(2), depth[k], p, un, vn, put)

    def put_second(t, r, ap, a, b):
        add_to_half(k, t, core[0], mine, theirs, 1, ap)

    adjoint_step(from_ref(h1), from_ref(u1), from_ref(v1), depth[k], p, un, vn, put_second)


def partials(body, name, core, gain, depth, state, scratch):
    halves = shape(2, HALF, GY)
    return pl.pallas_call(
        body,
        grid=(2,),
        in_specs=[SMEM, SMEM, SMEM, STATE],
        out_specs=[whole(2, HALF, GY)] * 2,
        out_shape=[halves, halves],
        scratch_shapes=scratch,
        compiler_params=params(),
        cost_estimate=cost(4, 4 << 20),
        name=name,
    )(core, gain, depth, state)


def join_columns(core, mine, other, total_depth, column, second):
    def first(t, r):
        s = pl.multiple_of((t % (CHUNKS // 2)) * R, R)

        @pl.when(t // (CHUNKS // 2) == core)
        def _():
            column[pl.ds(r, R), :] = mine[0, pl.ds(s, R), :]
            second[pl.ds(r, R), :] = mine[1, pl.ds(s, R), :]

        @pl.when(t // (CHUNKS // 2) != core)
        def _():
            column[pl.ds(r, R), :] = other[0, pl.ds(s, R), :]
            second[pl.ds(r, R), :] = other[1, pl.ds(s, R), :]

    clear_pads([column], [])
    over_rows(first)
    laplacian_onto(column, lambda r: second[pl.ds(r, R), :], total_depth, second)


def both_forward(x, column, second, gain, depth, p, un, vn, h1, u1, v1, put):
    field = lambda f: lambda r: x[f, 0, pl.ds(r, R), :]
    from_ref = lambda ref: lambda r: ref[pl.ds(r, R), :]

    def keep(t, r, h, u, v):
        h1[pl.ds(r, R), :] = h
        u1[pl.ds(r, R), :] = u
        v1[pl.ds(r, R), :] = v

    forward_step(field(0), field(1), field(2), from_ref(column), gain, depth, p, un, vn, keep)
    forward_step(from_ref(h1), from_ref(u1), from_ref(v1), from_ref(second), gain, depth, p, un, vn, put)


def both_adjoint(x, column, second, gain, depth, p, un, vn, h1, u1, v1, put):
    field = lambda f: lambda r: x[f, 0, pl.ds(r, R), :]
    from_ref = lambda ref: lambda r: ref[pl.ds(r, R), :]

    def keep(t, r, ap, u, v):
        h1[pl.ds(r, R), :] = x[0, 0, pl.ds(r, R), :] + gain * ap + COUP * column[pl.ds(r, R), :]
        u1[pl.ds(r, R), :] = u
        v1[pl.ds(r, R), :] = v

    def last(t, r, ap, u, v):
        put(t, r, h1[pl.ds(r, R), :] + gain * ap + COUP * second[pl.ds(r, R), :], u, v)

    adjoint_step(field(0), field(1), field(2), depth, p, un, vn, keep)
    adjoint_step(from_ref(h1), from_ref(u1), from_ref(v1), depth, p, un, vn, last)


COLUMN_SCRATCH = [pltpu.VMEM((GX + 8, GY), F32), pltpu.VMEM((GX, GY), F32)]
LEVEL_SCRATCH = [pltpu.VMEM((GX, GY), F32)] * 3
ANY = pl.BlockSpec(memory_space=pl.ANY)


def level_state(level):
    return pl.BlockSpec((3, 1, GX, GY), lambda i: (0, level, 0, 0))


def chain_terms_body(
    level, core, place, gain, depth, total, factor, x, lam, ev, mine, other, o0, o1, o2, o3,
    p, un, vn, h1, u1, v1, column, second, term,
):
    clear_pads([p], [un])
    join_columns(core[0], mine, other, total[0], column, second)

    def put(t, r, h, u, v):
        for f, moved in enumerate((h, u, v)):
            own = ev[f, 0, pl.ds(r, R), :] * lam[f, 0, pl.ds(r, R), :] + x[f, 0, pl.ds(r, R), :]
            term[f, pl.ds(r, R), :] = factor[f, level] * own - moved

    both_forward(x, column, second, gain[level], depth[level], p, un, vn, h1, u1, v1, put)
    for slot, out in enumerate((o0, o1, o2, o3)):
        r = pl.multiple_of(lax.rem(place[0] + slot, 4) * QUARTER, QUARTER)
        for f in range(3):
            out[f] = term[f, pl.ds(r, QUARTER), :]


def chain_terms(level, core, place, gain, depth, total, factor, x, lam, ev, mine, other):
    return pl.pallas_call(
        functools.partial(chain_terms_body, level),
        grid=(1,),
        in_specs=[SMEM] * 6 + [level_state(level)] * 3 + [whole(2, HALF, GY)] * 2,
        out_specs=[whole(3, QUARTER, GY)] * 4,
        out_shape=[shape(3, QUARTER, GY)] * 4,
        scratch_shapes=SCRATCH + LEVEL_SCRATCH + COLUMN_SCRATCH + [pltpu.VMEM((3, GX, GY), F32)],
        compiler_params=params(),
        cost_estimate=cost(4, 8 << 20),
        name="chain_terms",
    )(core, place, gain, depth, total, factor, x, lam, ev, mine, other)


def products_body(
    level, core, gain, depth, total, x, lam, ev, xr, lr, fm, fo, am, ao, added, *rest
):
    dual, block, p, un, vn, h1, u1, v1, column, second = rest[-10:]
    clear_pads([p], [un])
    join_columns(core[0], fm, fo, total[0], column, second)

    def put(t, r, h, u, v):
        for f, moved in enumerate((h, u, v)):
            own = ev[f, 0, pl.ds(r, R), :] * lam[f, 0, pl.ds(r, R), :] + x[f, 0, pl.ds(r, R), :]
            dual[f, 0, pl.ds(r, R), :] = own - moved

    both_forward(xr, column, second, gain[level], depth[level], p, un, vn, h1, u1, v1, put)
    join_columns(core[0], am, ao, total[0], column, second)

    def put_adjoint(t, r, h, u, v):
        block[0, 0, pl.ds(r, R), :] = (lam[0, 0, pl.ds(r, R), :] - h) + added[0, pl.ds(r, R), :]
        block[1, 0, pl.ds(r, R), :] = lam[1, 0, pl.ds(r, R), :] - u
        block[2, 0, pl.ds(r, R), :] = lam[2, 0, pl.ds(r, R), :] - v

    both_adjoint(lr, column, second, gain[level], depth[level], p, un, vn, h1, u1, v1, put_adjoint)


def products(level, core, gain, depth, total, x, lam, ev, xr, lr, fm, fo, am, ao, added, *earlier):
    state = shape(3, 2, GX, GY)
    return pl.pallas_call(
        functools.partial(products_body, level),
        grid=(1,),
        in_specs=[SMEM] * 4
        + [level_state(level)] * 3
        + [level_state(0)] * 2
        + [whole(2, HALF, GY)] * 4
        + [pl.BlockSpec((1, GX, GY), lambda i: (level, 0, 0))]
        + [ANY] * len(earlier),
        out_specs=[level_state(level)] * 2,
        out_shape=[state, state],
        input_output_aliases={14 + i: i for i in range(len(earlier))},
        scratch_shapes=SCRATCH + LEVEL_SCRATCH + COLUMN_SCRATCH,
        compiler_params=params(),
        cost_estimate=cost(6, 13 << 20),
        name="products",
    )(core, gain, depth, total, x, lam, ev, xr, lr, fm, fo, am, ao, added, *earlier)


PIECES = [whole(3, QUARTER, GY)] * 4
LINES = whole(8, 3, 8, GY)


def line_total_body(weights, a0, a1, a2, a3, out):
    for f in range(3):
        for i in range(8):
            rows = slice(8 * i, 8 * i + 8)
            sums = [weights[f, s] * a[f, rows, :] for s, a in enumerate((a0, a1, a2, a3))]
            out[i, f] = (sums[0] + sums[1]) + (sums[2] + sums[3])


def line_total(weights, pieces):
    return pl.pallas_call(
        line_total_body,
        grid=(1,),
        in_specs=[SMEM] + PIECES,
        out_specs=LINES,
        out_shape=shape(8, 3, 8, GY),
        compiler_params=params(),
        cost_estimate=cost(1, 2 << 20),
        name="line_total",
    )(weights, *pieces)


def scan_lines_body(factors, terms, out):
    for f in range(3):
        carry = jnp.zeros((8, GY), F32)
        for line in range(8):
            out[line, f] = carry
            if line < 7:
                carry = factors[line, f] * carry + terms[line, f]


def scan_lines(factors, terms):
    return pl.pallas_call(
        scan_lines_body,
        grid=(1,),
        in_specs=[SMEM, LINES],
        out_specs=LINES,
        out_shape=shape(8, 3, 8, GY),
        compiler_params=params(),
        cost_estimate=cost(1, 1 << 20),
        name="scan_lines",
    )(factors, terms)


def spread_body(weights, carried, a0, a1, a2, a3, o0, o1, o2, o3):
    for f in range(3):
        for i in range(8):
            rows = slice(8 * i, 8 * i + 8)
            terms = [a[f, rows, :] for a in (a0, a1, a2, a3)] + [carried[i, f]]
            for slot, out in enumerate((o0, o1, o2, o3)):
                parts = [weights[f, slot, s] * term for s, term in enumerate(terms)]
                out[f, rows, :] = ((parts[0] + parts[1]) + (parts[2] + parts[3])) + parts[4]


def spread(weights, carried, pieces):
    return pl.pallas_call(
        spread_body,
        grid=(1,),
        in_specs=[SMEM, LINES] + PIECES,
        out_specs=PIECES,
        out_shape=[shape(3, QUARTER, GY)] * 4,
        compiler_params=params(),
        cost_estimate=cost(1, 4 << 20),
        name="spread",
    )(weights, carried, *pieces)


def finish_body(place, x, lam, ev, a0, a1, a2, a3, *rest):
    out = rest[-1]
    for slot, part in enumerate((a0, a1, a2, a3)):
        r = pl.multiple_of(lax.rem(place[0] + slot, 4) * QUARTER, QUARTER)
        for f in range(3):
            rows = pl.ds(r, QUARTER)
            out[f, 0, rows, :] = (ev[f, 0, rows, :] * lam[f, 0, rows, :] + x[f, 0, rows, :]) + part[f]


def finish(level, place, x, lam, ev, parts, *earlier):
    return pl.pallas_call(
        finish_body,
        grid=(1,),
        in_specs=[SMEM] + [level_state(level)] * 3 + PIECES + [ANY] * len(earlier),
        out_specs=level_state(level),
        out_shape=shape(3, 2, GX, GY),
        input_output_aliases={8: 0} if earlier else {},
        compiler_params=params(),
        cost_estimate=cost(3, 8 << 20),
        name="finish",
    )(place, x, lam, ev, *parts, *earlier)


LEVELS_HERE = 2
LINE = 4


def along(axis, distance):
    size = lax.axis_size(axis)
    return [(i, i + distance) for i in range(size) if 0 <= i + distance < size]


def swap(array, bit):
    return lax.ppermute(array, "lev", [(i, i ^ bit) for i in range(lax.axis_size("lev"))])


def around(array, distance):
    size = lax.axis_size("tm")
    return lax.ppermute(
        array, "tm", [(i, i - i % LINE + (i % LINE + distance) % LINE) for i in range(size)]
    )


def across(array):
    size = lax.axis_size("tm")
    groups = [list(range(place, size, LINE)) for place in range(LINE)]
    return lax.all_to_all(array, "tm", 0, 0, tiled=True, axis_index_groups=groups)


def chain_weights(factors, slab):
    ahead = jnp.concatenate([factors[1:], jnp.zeros((1, 6), F32)])
    lines = ahead.reshape(-1, LINE, 6)
    whole_lines = jnp.prod(lines, axis=1)
    here = lax.dynamic_index_in_dim(lines, slab // LINE, keepdims=False)
    one, nil = jnp.ones((6,), F32), jnp.zeros((6,), F32)

    def product(first, last):
        out = one
        for i in range(first, last):
            out = out * here[i]
        return out

    table = jnp.stack(
        [
            jnp.stack([product(t + 1, j) if t < j else nil for t in range(LINE)] + [product(0, j)])
            for j in range(LINE + 1)
        ]
    )
    place = slab % LINE
    slots = (jnp.arange(LINE) + place) % LINE
    by_slot = table[:, jnp.concatenate([slots, jnp.array([LINE])])]
    own = lax.dynamic_index_in_dim(ahead, slab, keepdims=False)
    return own, by_slot[LINE, :LINE], by_slot[slots], whole_lines


def shards(
    increment, multiplier, error_var, obs_cell, obs_dual, obs_var, level_gain, mean_depth, chain_decay
):
    x, lam, ev = increment[0], multiplier[0], error_var[0]
    lev = lax.axis_index("lev")
    core, ylo = lev % 2, lev // 2
    core_arr = core.astype(jnp.int32).reshape(1)
    slab = lax.axis_index("tm")
    place = (slab % LINE).astype(jnp.int32).reshape(1)

    raw = []
    for k in range(LEVELS_HERE):
        with jax.named_scope(f"raw{k}x"):
            xr = lax.ppermute(x[:, k : k + 1], "tm", along("tm", 1))
        with jax.named_scope(f"raw{k}l"):
            lr = lax.ppermute(lam[:, k : k + 1], "tm", along("tm", -1))
        raw.append((xr, lr))

    total = jnp.sum(mean_depth).reshape(1)
    total = total + swap(total, 1)
    total = total + swap(total, 2)
    mine = chain_decay[0].reshape(6)
    with jax.named_scope("decays"):
        factors = lax.all_to_all(jnp.broadcast_to(mine, (32, 6)), "tm", 0, 0, tiled=True)
    own, to_total, to_slots, whole_lines = chain_weights(factors, slab)
    own = own.reshape(3, 2)

    with jax.named_scope("fpart"):
        fm, ft = partials(
            forward_partials_body, "forward_partials", core_arr, level_gain, mean_depth, x, SCRATCH
        )
    with jax.named_scope("fs1"):
        fm = fm + swap(ft, 1)
    with jax.named_scope("fs2"):
        fm = fm + swap(fm, 2)
    with jax.named_scope("fs3"):
        fo = swap(fm, 1)
    with jax.named_scope("apart"):
        am, at = partials(
            adjoint_partials_body, "adjoint_partials", core_arr, level_gain, mean_depth, lam, SCRATCH + LEVEL_SCRATCH
        )
    with jax.named_scope("as1"):
        am = am + swap(at, 1)
    with jax.named_scope("as2"):
        am = am + swap(am, 2)

    chain = ()
    for k in range(LEVELS_HERE):
        with jax.named_scope(f"terms{k}"):
            pieces = chain_terms(
                k, core_arr, place, level_gain, mean_depth, total, own, x, lam, ev, fm, fo
            )
        with jax.named_scope(f"in{k}"):
            pieces = [pieces[0], around(pieces[3], -1), around(pieces[2], 2), around(pieces[1], 1)]
        pick = lambda a: a.reshape(a.shape[:-1] + (3, 2))[..., k]
        sums = line_total(jnp.moveaxis(pick(to_total), -1, 0), pieces)
        with jax.named_scope(f"acrossin{k}"):
            lines = across(sums)
        lines = scan_lines(pick(whole_lines), lines)
        with jax.named_scope(f"acrossout{k}"):
            carried = across(lines)
        parts = spread(jnp.moveaxis(pick(to_slots), -1, 0), carried, pieces)
        with jax.named_scope(f"out{k}"):
            parts = [parts[0], around(parts[3], -1), around(parts[2], 2), around(parts[1], 1)]
        chain = (finish(k, place, x, lam, ev, parts, *chain),)

    quarter = HALF // 2
    with jax.named_scope("colz"):
        fq = lax.ppermute(lax.dynamic_slice_in_dim(fm, ylo * quarter, quarter, 1), "tm", along("tm", 1))
        aq = lax.ppermute(lax.dynamic_slice_in_dim(am, ylo * quarter, quarter, 1), "tm", along("tm", -1))
    q = jnp.concatenate([fq, aq])
    with jax.named_scope("coly"):
        qo = swap(q, 2)
    half = jnp.where(ylo == 0, jnp.concatenate([q, qo], 1), jnp.concatenate([qo, q], 1))
    with jax.named_scope("colc"):
        other = swap(half, 1)

    rows, cols = obs_cell[0] // GY, obs_cell[0] % GY
    level = lax.broadcasted_iota(jnp.int32, rows.shape, 0)
    obs_product = obs_var[0] * obs_dual[0] + x[0][level, rows, cols]
    added = jnp.zeros(x[0].shape, F32).at[level, rows, cols].add(obs_dual[0])

    done = ()
    for k in range(LEVELS_HERE):
        done = products(
            k, core_arr, level_gain, mean_depth, total, x, lam, ev, *raw[k],
            half[:2], other[:2], half[2:], other[2:], added, *done,
        )
    dual, block = done
    return dual[None], obs_product[None], block[None], chain[0][None]


def solution(mesh):
    state = P("tm", None, "lev", None, None)
    obs = P("tm", "lev", None)
    return jax.shard_map(
        shards,
        mesh=mesh,
        in_specs=(state, state, state, obs, obs, obs, P("lev"), P("lev"), P("tm", None, "lev")),
        out_specs=(state, obs, state, state),
        check_vma=False,
    )
```

```python
import jax
import jax.numpy as jnp
from jax import lax
from jax.experimental import pallas as pl
from jax.experimental.pallas import tpu as pltpu
from jax.sharding import PartitionSpec as P


DT = 0.25
ROT = 0.5
COUP = 0.25
LINE = 4
GX, GY = 256, 512
HALF = GX // 2
SENT = HALF + 8
R = 128
CHUNKS = GX // R
F32 = jnp.float32


def shape(*dims):
    return jax.ShapeDtypeStruct(dims, F32)


def over_rows(body):
    def step(t, carry):
        body(t, pl.multiple_of(t * R, R))
        return carry

    lax.fori_loop(0, CHUNKS, step, 0, unroll=True)


def lanes():
    return lax.broadcasted_iota(jnp.int32, (R, GY), 1)


def next_lane(a):
    return jnp.where(lanes() < GY - 1, pltpu.roll(a, GY - 1, 1), 0.0)


def prev_lane(a):
    return jnp.where(lanes() > 0, pltpu.roll(a, 1, 1), 0.0)


def rows_and_next(ref, r):
    big = ref[pl.ds(r, R + 8), :]
    return big[:R], pltpu.roll(big, R + 7, 0)[:R]


def rows_and_prev(ref, r):
    big = ref[pl.ds(r, R + 8), :]
    return big[8:], pltpu.roll(big, 1, 0)[8:]


def clear_pads(nxt, prv):
    for ref in nxt:
        ref[GX : GX + 8, :] = jnp.zeros((8, GY), F32)
    for ref in prv:
        ref[0:8, :] = jnp.zeros((8, GY), F32)


def forward_step(h, u, v, column, gain, depth, p, un, vn, put):
    def first(t, r):
        here = gain * h(r)
        p[pl.ds(r, R), :] = here if column is None else here + COUP * column(r)

    over_rows(first)

    def second(t, r):
        here, after = rows_and_next(p, r)
        u0, v0 = u(r), v(r)
        un[pl.ds(r + 8, R), :] = u0 + DT * (ROT * v0 - (after - here))
        vn[pl.ds(r, R), :] = v0 - DT * (ROT * u0 + (next_lane(here) - here))

    over_rows(second)

    def third(t, r):
        u1, before = rows_and_prev(un, r)
        v1 = vn[pl.ds(r, R), :]
        put(t, r, h(r) - DT * depth * ((u1 - before) + (v1 - prev_lane(v1))), u1, v1)

    over_rows(third)


def adjoint_step(h, u, v, depth, p, un, vn, put):
    def first(t, r):
        p[pl.ds(r, R), :] = h(r)

    over_rows(first)

    def second(t, r):
        here, after = rows_and_next(p, r)
        un[pl.ds(r + 8, R), :] = u(r) + DT * depth * (after - here)
        vn[pl.ds(r, R), :] = v(r) + DT * depth * (next_lane(here) - here)

    over_rows(second)

    def third(t, r):
        u1, before = rows_and_prev(un, r)
        v1 = vn[pl.ds(r, R), :]
        put(t, r, DT * ((u1 - before) + (v1 - prev_lane(v1))), u1 - DT * ROT * v1, v1 + DT * ROT * u1)

    over_rows(third)


def laplacian_onto(column, extra, total_depth, target):
    def body(t, r):
        here, after = rows_and_next(column, r)
        dx = after - here
        start = jnp.maximum(r - 8, 0)
        edge = column[pl.ds(pl.multiple_of(start, 8), 8), :][7:8]
        rows = lax.broadcasted_iota(jnp.int32, (R, GY), 0)
        before = jnp.where(rows == 0, edge, pltpu.roll(here, 1, 0))
        back = jnp.where(rows + r > 0, here - before, 0.0)
        dy = next_lane(here) - here
        target[pl.ds(r, R), :] = extra(r) + (DT * DT * COUP * total_depth) * ((dx - back) + (dy - prev_lane(dy)))

    over_rows(body)


SCRATCH = [pltpu.VMEM((GX + 8, GY), F32), pltpu.VMEM((GX + 8, GY), F32), pltpu.VMEM((GX, GY), F32)]
STATE = pl.BlockSpec((3, 1, GX, GY), lambda k: (0, k, 0, 0))
QUARTER = GX // 4
SMEM = pl.BlockSpec(memory_space=pltpu.SMEM)


def whole(*dims):
    return pl.BlockSpec(dims, lambda k: (0,) * len(dims))


def cost(micros, moved):
    return pl.CostEstimate(flops=int(micros * 4_000_000), bytes_accessed=moved, transcendentals=0)


def params():
    return pltpu.CompilerParams(dimension_semantics=("arbitrary",), vmem_limit_bytes=67_043_328)


def add_to_half(k, t, core, mine, theirs, slot, value):
    r = pl.multiple_of((t % (CHUNKS // 2)) * R, R)

    def onto(ref):
        @pl.when(k == 0)
        def _():
            ref[slot, pl.ds(r, R), :] = value

        @pl.when(k > 0)
        def _():
            ref[slot, pl.ds(r, R), :] += value

    pl.when(t // (CHUNKS // 2) == core)(lambda: onto(mine))
    pl.when(t // (CHUNKS // 2) != core)(lambda: onto(theirs))


def put_depths(k, depth, *outs):
    @pl.when(k == 0)
    def _():
        for out in outs:
            for slot in range(2):
                out[slot, HALF:SENT, :] = jnp.full((8, GY), depth[0] + depth[1], F32)


def forward_partials_body(core, gain, depth, x, mine, theirs, p, un, vn):
    k = pl.program_id(0)
    put_depths(k, depth, mine, theirs)
    clear_pads([p], [un])

    def put(t, r, h1, u1, v1):
        add_to_half(k, t, core[0], mine, theirs, 0, x[0, 0, pl.ds(r, R), :])
        add_to_half(k, t, core[0], mine, theirs, 1, h1)

    field = lambda f: lambda r: x[f, 0, pl.ds(r, R), :]
    forward_step(field(0), field(1), field(2), None, gain[k], depth[k], p, un, vn, put)


def adjoint_partials_body(core, gain, depth, x, mine, theirs, p, un, vn, h1, u1, v1):
    k = pl.program_id(0)
    put_depths(k, depth, mine, theirs)
    clear_pads([p], [un])
    field = lambda f: lambda r: x[f, 0, pl.ds(r, R), :]
    from_ref = lambda ref: lambda r: ref[pl.ds(r, R), :]

    def put(t, r, ap, a, b):
        add_to_half(k, t, core[0], mine, theirs, 0, ap)
        h1[pl.ds(r, R), :] = x[0, 0, pl.ds(r, R), :] + gain[k] * ap
        u1[pl.ds(r, R), :] = a
        v1[pl.ds(r, R), :] = b

    adjoint_step(field(0), field(1), field(2), depth[k], p, un, vn, put)

    def put_second(t, r, ap, a, b):
        add_to_half(k, t, core[0], mine, theirs, 1, ap)

    adjoint_step(from_ref(h1), from_ref(u1), from_ref(v1), depth[k], p, un, vn, put_second)


def partials(body, core, gain, depth, state, scratch):
    halves = shape(2, SENT, GY)
    return pl.pallas_call(
        body,
        grid=(2,),
        in_specs=[SMEM, SMEM, SMEM, STATE],
        out_specs=[whole(2, SENT, GY)] * 2,
        out_shape=[halves, halves],
        scratch_shapes=scratch,
        compiler_params=params(),
        cost_estimate=cost(4, 4 << 20),
    )(core, gain, depth, state)


def join_columns(core, mine, other, total_depth, column, second):
    def first(t, r):
        s = pl.multiple_of((t % (CHUNKS // 2)) * R, R)

        @pl.when(t // (CHUNKS // 2) == core)
        def _():
            column[pl.ds(r, R), :] = mine[0, pl.ds(s, R), :]
            second[pl.ds(r, R), :] = mine[1, pl.ds(s, R), :]

        @pl.when(t // (CHUNKS // 2) != core)
        def _():
            column[pl.ds(r, R), :] = other[0, pl.ds(s, R), :]
            second[pl.ds(r, R), :] = other[1, pl.ds(s, R), :]

    clear_pads([column], [])
    over_rows(first)
    laplacian_onto(column, lambda r: second[pl.ds(r, R), :], total_depth, second)


def both_forward(x, column, second, gain, depth, p, un, vn, h1, u1, v1, put):
    field = x if callable(x) else lambda f: lambda r: x[f, 0, pl.ds(r, R), :]
    from_ref = lambda ref: lambda r: ref[pl.ds(r, R), :]

    def keep(t, r, h, u, v):
        h1[pl.ds(r, R), :] = h
        u1[pl.ds(r, R), :] = u
        v1[pl.ds(r, R), :] = v

    forward_step(field(0), field(1), field(2), from_ref(column), gain, depth, p, un, vn, keep)
    forward_step(from_ref(h1), from_ref(u1), from_ref(v1), from_ref(second), gain, depth, p, un, vn, put)


def both_adjoint(x, column, second, gain, depth, p, un, vn, h1, u1, v1, put):
    field = x if callable(x) else lambda f: lambda r: x[f, 0, pl.ds(r, R), :]
    from_ref = lambda ref: lambda r: ref[pl.ds(r, R), :]

    def keep(t, r, ap, u, v):
        h1[pl.ds(r, R), :] = field(0)(r) + gain * ap + COUP * column[pl.ds(r, R), :]
        u1[pl.ds(r, R), :] = u
        v1[pl.ds(r, R), :] = v

    def last(t, r, ap, u, v):
        put(t, r, h1[pl.ds(r, R), :] + gain * ap + COUP * second[pl.ds(r, R), :], u, v)

    adjoint_step(field(0), field(1), field(2), depth, p, un, vn, keep)
    adjoint_step(from_ref(h1), from_ref(u1), from_ref(v1), depth, p, un, vn, last)


COLUMN_SCRATCH = [pltpu.VMEM((GX + 8, GY), F32), pltpu.VMEM((GX, GY), F32)]
LEVEL_SCRATCH = [pltpu.VMEM((GX, GY), F32)] * 3
ANY = pl.BlockSpec(memory_space=pl.ANY)


def chain_terms_body(
    core, place, gain, depth, factor, x, lam, ev, mine, other, own_rows, *rest
):
    outs, (p, un, vn, h1, u1, v1, column, second, term) = rest[:LINE], rest[LINE:]
    k = pl.program_id(0)

    @pl.when(k == 0)
    def _():
        clear_pads([p], [un])
        join_columns(core[0], mine, other, mine[0, HALF : HALF + 1, :], column, second)

    def put(t, r, h, u, v):
        for f, moved in enumerate((h, u, v)):
            own = ev[f, 0, pl.ds(r, R), :] * lam[f, 0, pl.ds(r, R), :] + x[f, 0, pl.ds(r, R), :]
            own_rows[f, 0, pl.ds(r, R), :] = own
            term[f, pl.ds(r, R), :] = factor[2 * f + k] * own - moved

    both_forward(x, column, second, gain[k], depth[k], p, un, vn, h1, u1, v1, put)
    for slot, out in enumerate(outs):
        r = pl.multiple_of(lax.rem(place[0] + slot, LINE) * QUARTER, QUARTER)
        for f in range(3):
            out[0, f] = term[f, pl.ds(r, QUARTER), :]


def by_level(*dims):
    return pl.BlockSpec((1,) + dims, lambda k: (k,) + (0,) * len(dims))


PIECES = [by_level(3, QUARTER, GY)] * LINE
PIECE_SHAPES = [shape(2, 3, QUARTER, GY)] * LINE


def chain_terms(core, place, gain, depth, factor, x, lam, ev, mine, other):
    return pl.pallas_call(
        chain_terms_body,
        grid=(2,),
        in_specs=[SMEM] * 5 + [STATE] * 3 + [whole(2, SENT, GY)] * 2,
        out_specs=[STATE] + PIECES,
        out_shape=[shape(3, 2, GX, GY)] + PIECE_SHAPES,
        scratch_shapes=SCRATCH + LEVEL_SCRATCH + COLUMN_SCRATCH + [pltpu.VMEM((3, GX, GY), F32)],
        compiler_params=params(),
        cost_estimate=cost(7, 16 << 20),
        name="chain_terms",
    )(core, place, gain, depth, factor, x, lam, ev, mine, other)


def columns_of(model):
    return pl.BlockSpec((2, HALF, GY), lambda k: (model, 0, 0))


def products_body(
    core, second_way, gain, depth, depths, own, lam, xr, xr2, xv, xv2, lr, lr2, lv, lv2, fm, fo, am, ao, added,
    dual, block, p, un, vn, h1, u1, v1, fc, fs, ac, as_,
):
    k = pl.program_id(0)

    @pl.when(k == 0)
    def _():
        clear_pads([p], [un])
        join_columns(core[0], fm, fo, depths[0, 0:1, :], fc, fs)
        join_columns(core[0], am, ao, depths[0, 0:1, :], ac, as_)

    def arrived(first, second, last, second_last, flag):
        def field(f):
            a, b, i, at = (first, second, f, flag) if f < SENT_FIRST else (last, second_last, f - SENT_FIRST, flag + 1)
            return lambda r: jnp.where(second_way[at] > 0, b[i, 0, pl.ds(r, R), :], a[i, 0, pl.ds(r, R), :])

        return field

    def put(t, r, h, u, v):
        for f, moved in enumerate((h, u, v)):
            dual[f, 0, pl.ds(r, R), :] = own[f, 0, pl.ds(r, R), :] - moved

    both_forward(arrived(xr, xr2, xv, xv2, 0), fc, fs, gain[k], depth[k], p, un, vn, h1, u1, v1, put)

    def put_adjoint(t, r, h, u, v):
        block[0, 0, pl.ds(r, R), :] = (lam[0, 0, pl.ds(r, R), :] - h) + added[0, pl.ds(r, R), :]
        block[1, 0, pl.ds(r, R), :] = lam[1, 0, pl.ds(r, R), :] - u
        block[2, 0, pl.ds(r, R), :] = lam[2, 0, pl.ds(r, R), :] - v

    both_adjoint(arrived(lr, lr2, lv, lv2, 2), ac, as_, gain[k], depth[k], p, un, vn, h1, u1, v1, put_adjoint)


SENT_FIRST = 2


def fields(count):
    return pl.BlockSpec((count, 1, GX, GY), lambda k: (0, k, 0, 0))


def products(core, second_way, gain, depth, depths, own, lam, arrivals, fm, fo, am, ao, added):
    state = shape(3, 2, GX, GY)
    return pl.pallas_call(
        products_body,
        grid=(2,),
        in_specs=[SMEM] * 4
        + [pl.BlockSpec((1, 8, GY), lambda k: (0, HALF // 8, 0))]
        + [STATE] * 2
        + [fields(SENT_FIRST), fields(SENT_FIRST), fields(3 - SENT_FIRST), fields(3 - SENT_FIRST)] * 2
        + [columns_of(0), columns_of(0), columns_of(1), columns_of(1)]
        + [pl.BlockSpec((1, GX, GY), lambda k: (k, 0, 0))],
        out_specs=[STATE] * 2,
        out_shape=[state, state],
        scratch_shapes=SCRATCH + LEVEL_SCRATCH + COLUMN_SCRATCH * 2,
        compiler_params=params(),
        cost_estimate=cost(12, 24 << 20),
        name="products",
    )(core, second_way, gain, depth, depths, own, lam, *arrivals, fm, fo, am, ao, added)


SUB = QUARTER // LINE
PACKED = 3 * SUB + 8
PARTS = [by_level(PACKED, GY)] * LINE
CARRIES = by_level(3 * SUB, GY)


def in_place_order(place, pieces, ordered):
    for slot, piece in enumerate(pieces):
        ordered[lax.rem(place[0] + slot, LINE)] = piece[0]


def factor_after(place, slots, level, f, j):
    slot = lax.rem(j - place[0] + LINE, LINE)
    values = [ref[2 * f + level] for ref in slots]
    return jnp.where(slot < 2, jnp.where(slot == 0, values[0], values[1]), jnp.where(slot == 2, values[2], values[3]))


def line_total_body(place, line, d0, d1, d2, d3, a0, a1, a2, a3, *rest):
    outs, ordered = rest[:LINE], rest[LINE]
    level = pl.program_id(0)
    in_place_order(place, (a0, a1, a2, a3), ordered)
    rows = lax.broadcasted_iota(jnp.int32, (8, GY), 0)
    plane = jnp.zeros((8, GY), F32)
    for f in range(3):
        factors = [factor_after(place, (d0, d1, d2, d3), level, f, j) for j in range(LINE)]
        plane = jnp.where(rows == f, (factors[0] * factors[1]) * (factors[2] * factors[3]), plane)
        for slot, out in enumerate(outs):
            r = pl.multiple_of(lax.rem(line[0] + slot, LINE) * SUB, SUB)
            value = ordered[0, f, pl.ds(r, SUB), :]
            for j in range(1, LINE):
                value = factors[j] * value + ordered[j, f, pl.ds(r, SUB), :]
            out[0, SUB * f : SUB * f + SUB, :] = value
    for out in outs:
        out[0, 3 * SUB :, :] = plane


ORDERED = pltpu.VMEM((LINE, 3, QUARTER, GY), F32)


def line_total(place, line, factors, pieces):
    return pl.pallas_call(
        line_total_body,
        grid=(2,),
        in_specs=[SMEM] * (2 + LINE) + PIECES,
        out_specs=PARTS,
        out_shape=[shape(2, PACKED, GY)] * LINE,
        scratch_shapes=[ORDERED],
        compiler_params=params(),
        cost_estimate=cost(1, 2 << 20),
        name="line_total",
    )(place, line, *factors, *pieces)


def lines_onward(carry, ordered, f):
    out = [carry]
    for j in range(LINE):
        factor = ordered[j, 3 * SUB + f : 3 * SUB + f + 1, :]
        out.append(factor * out[-1] + ordered[j, SUB * f : SUB * f + SUB, :])
    return out


def put_in_order(line, parts, ordered):
    for slot, part in enumerate(parts):
        ordered[lax.rem(line[0] + slot, LINE)] = part[0]


def half_total_body(line, a0, a1, a2, a3, out, ordered):
    put_in_order(line, (a0, a1, a2, a3), ordered)
    for f in range(3):
        out[0, SUB * f : SUB * f + SUB, :] = lines_onward(jnp.zeros((SUB, GY), F32), ordered, f)[LINE]


def half_total(line, parts):
    return pl.pallas_call(
        half_total_body,
        grid=(2,),
        in_specs=[SMEM] + PARTS,
        out_specs=CARRIES,
        out_shape=shape(2, 3 * SUB, GY),
        scratch_shapes=[pltpu.VMEM((LINE, PACKED, GY), F32)],
        compiler_params=params(),
        cost_estimate=cost(1, 1 << 20),
        name="half_total",
    )(line, *parts)


def line_carries_body(line, carried, a0, a1, a2, a3, o0, o1, o2, o3, ordered, carries):
    put_in_order(line, (a0, a1, a2, a3), ordered)
    for f in range(3):
        rows = slice(SUB * f, SUB * f + SUB)
        for j, value in enumerate(lines_onward(carried[0, rows, :], ordered, f)[:LINE]):
            carries[j, rows, :] = value
    for slot, out in enumerate((o0, o1, o2, o3)):
        out[0] = carries[lax.rem(line[0] + slot, LINE)]


def line_carries(line, carried, parts):
    return pl.pallas_call(
        line_carries_body,
        grid=(2,),
        in_specs=[SMEM, CARRIES] + PARTS,
        out_specs=[CARRIES] * LINE,
        out_shape=[shape(2, 3 * SUB, GY)] * LINE,
        scratch_shapes=[pltpu.VMEM((LINE, PACKED, GY), F32), pltpu.VMEM((LINE, 3 * SUB, GY), F32)],
        compiler_params=params(),
        cost_estimate=cost(1, 1 << 20),
        name="line_carries",
    )(line, carried, *parts)


def spread_body(place, line, d0, d1, d2, d3, c0, c1, c2, c3, a0, a1, a2, a3, o0, o1, o2, o3, ordered):
    level = pl.program_id(0)
    in_place_order(place, (a0, a1, a2, a3), ordered)
    for f in range(3):
        factors = [factor_after(place, (d0, d1, d2, d3), level, f, j) for j in range(LINE)]
        for part, carried in enumerate((c0, c1, c2, c3)):
            r = pl.multiple_of(lax.rem(line[0] + part, LINE) * SUB, SUB)
            value = carried[0, SUB * f : SUB * f + SUB, :]
            for j in range(LINE):
                term = ordered[j, f, pl.ds(r, SUB), :]
                ordered[j, f, pl.ds(r, SUB), :] = value
                value = factors[j] * value + term
    for slot, out in enumerate((o0, o1, o2, o3)):
        out[0] = ordered[lax.rem(place[0] + slot, LINE)]


def spread(place, line, factors, carried, pieces):
    return pl.pallas_call(
        spread_body,
        grid=(2,),
        in_specs=[SMEM] * (2 + LINE) + [CARRIES] * LINE + PIECES,
        out_specs=PIECES,
        out_shape=PIECE_SHAPES,
        scratch_shapes=[ORDERED],
        compiler_params=params(),
        cost_estimate=cost(1, 4 << 20),
        name="spread",
    )(place, line, *factors, *carried, *pieces)


def finish_body(place, own, a0, a1, a2, a3, out):
    for slot, part in enumerate((a0, a1, a2, a3)):
        rows = pl.ds(pl.multiple_of(lax.rem(place[0] + slot, LINE) * QUARTER, QUARTER), QUARTER)
        for f in range(3):
            out[f, 0, rows, :] = own[f, 0, rows, :] + part[0, f]


def finish(place, own, parts):
    return pl.pallas_call(
        finish_body,
        grid=(2,),
        in_specs=[SMEM, STATE] + PIECES,
        out_specs=STATE,
        out_shape=shape(3, 2, GX, GY),
        compiler_params=params(),
        cost_estimate=cost(5, 9 << 20),
        name="finish",
    )(place, own, *parts)


def along(axis, distance):
    size = lax.axis_size(axis)
    return [(i, i + distance) for i in range(size) if 0 <= i + distance < size]


def swap(array, bit):
    return lax.ppermute(array, "lev", [(i, i ^ bit) for i in range(lax.axis_size("lev"))])


def around(array, distance):
    size = lax.axis_size("tm")
    return lax.ppermute(
        array, "tm", [(i, i - i % LINE + (i % LINE + distance) % LINE) for i in range(size)]
    )


def sideways(array, distance):
    size, four = lax.axis_size("tm"), LINE * LINE
    return lax.ppermute(
        array, "tm", [(i, i - i % four + (i % four + LINE * distance) % four) for i in range(size)]
    )


def to_second_half(array):
    half = lax.axis_size("tm") // 2
    return lax.ppermute(array, "tm", [(i, i + half) for i in range(half)])


def shards(
    increment, multiplier, error_var, obs_cell, obs_dual, obs_var, level_gain, mean_depth, chain_decay
):
    x, lam, ev = increment[0], multiplier[0], error_var[0]
    lev = lax.axis_index("lev")
    core, ylo = lev % 2, lev // 2
    core_arr = core.astype(jnp.int32).reshape(1)
    slab = lax.axis_index("tm")
    place = (slab % LINE).astype(jnp.int32).reshape(1)

    def exchanged(pieces, move=around):
        out = [pieces[0]]
        for slot, distance in ((3, -1), (2, 2), (1, 1)):
            out.append(move(pieces[slot], distance))
        return out

    own = lax.ppermute(chain_decay[0].reshape(6), "tm", along("tm", -1))
    size = lax.axis_size("tm")
    mid, half_ring = size // 2, lambda d: [(i, i - i % mid + (i % mid + d) % mid) for i in range(size)]
    arrivals = []
    for array, step in ((x, 1), (lam, -1)):
        ends = (0, mid) if step > 0 else (mid - 1, size - 1)
        first = lax.ppermute(array[:SENT_FIRST], "tm", half_ring(step))
        first_2 = lax.ppermute(first, "tm", [ends if step > 0 else ends[::-1]])
        last = around(array[SENT_FIRST:], step)
        hops = [(i, i + LINE * step) for i in range(0 if step > 0 else LINE - 1, size, LINE)]
        last_2 = lax.ppermute(last, "tm", [(i, j) for i, j in hops if 0 <= j < size])
        arrivals += [first, first_2, last, last_2]
    second_way = jnp.stack(
        [slab % mid == 0, slab % LINE == 0, slab % mid == mid - 1, slab % LINE == LINE - 1]
    ).astype(jnp.int32)
    here = exchanged([own] * LINE)
    fm, ft = partials(forward_partials_body, core_arr, level_gain, mean_depth, x, SCRATCH)
    fm = fm + swap(ft, 1)
    fm = fm + swap(fm, 2)
    fo = swap(fm, 1)
    am, at = partials(adjoint_partials_body, core_arr, level_gain, mean_depth, lam, SCRATCH + LEVEL_SCRATCH)
    am = am + swap(at, 1)
    am = am + swap(am, 2)

    own_rows, *terms = chain_terms(
        core_arr, place, level_gain, mean_depth, own, x, lam, ev, fm, fo
    )
    cells, duals, terms[0] = lax.optimization_barrier((obs_cell[0], obs_dual[0], terms[0]))
    rows, cols = cells // GY, cells % GY
    level = lax.broadcasted_iota(jnp.int32, rows.shape, 0)
    obs_product = obs_var[0] * duals + x[jnp.zeros_like(level), level, rows, cols]
    added = jnp.zeros(x[0].shape, F32).at[level, rows, cols].add(duals)

    line = (slab // LINE % LINE).astype(jnp.int32).reshape(1)
    pieces = exchanged(terms)
    pieces[0], added = lax.optimization_barrier((pieces[0], added))
    sums = line_total(place, line, here, pieces)
    sums = exchanged(sums, sideways)
    carried = to_second_half(half_total(line, sums))
    carries = line_carries(line, carried, sums)
    carries = exchanged(carries, sideways)
    parts = spread(place, line, here, carries, pieces)
    parts = exchanged(parts)
    chain = finish(place, own_rows, parts)

    quarter = HALF // 2
    fq = lax.ppermute(
        lax.dynamic_slice_in_dim(fm, ylo * quarter, quarter, 1), "tm", along("tm", 1)
    )
    aq = lax.ppermute(lax.dynamic_slice_in_dim(am, ylo * quarter, quarter, 1), "tm", along("tm", -1))
    q = jnp.concatenate([fq, aq])
    qo = swap(q, 2)
    half = jnp.where(ylo == 0, jnp.concatenate([q, qo], 1), jnp.concatenate([qo, q], 1))
    other = swap(half, 1)

    dual, block = products(
        core_arr, second_way, level_gain, mean_depth, fm, own_rows, lam, arrivals,
        half, other, half, other, added,
    )
    return dual[None], obs_product[None], block[None], chain[None]


def solution(mesh):
    state = P("tm", None, "lev", None, None)
    obs = P("tm", "lev", None)

    return jax.shard_map(
        shards,
        mesh=mesh,
        in_specs=(state, state, state, obs, obs, obs, P("lev"), P("lev"), P("tm", None, "lev")),
        out_specs=(state, obs, state, state),
        check_vma=False,
    )
```

```python
import jax
import jax.numpy as jnp
from jax import lax
from jax.experimental import pallas as pl
from jax.experimental.pallas import tpu as pltpu
from jax.sharding import PartitionSpec as P


DT = 0.25
ROT = 0.5
COUP = 0.25
LINE = 4
GX, GY = 256, 512
HALF = GX // 2
SENT = HALF + 8
R = 128
CHUNKS = GX // R
F32 = jnp.float32


def shape(*dims):
    return jax.ShapeDtypeStruct(dims, F32)


def over_rows(body):
    def step(t, carry):
        body(t, pl.multiple_of(t * R, R))
        return carry

    lax.fori_loop(0, CHUNKS, step, 0, unroll=True)


def lanes():
    return lax.broadcasted_iota(jnp.int32, (R, GY), 1)


def next_lane(a):
    return jnp.where(lanes() < GY - 1, pltpu.roll(a, GY - 1, 1), 0.0)


def prev_lane(a):
    return jnp.where(lanes() > 0, pltpu.roll(a, 1, 1), 0.0)


def rows_and_next(ref, r):
    big = ref[pl.ds(r, R + 8), :]
    return big[:R], pltpu.roll(big, R + 7, 0)[:R]


def rows_and_prev(ref, r):
    big = ref[pl.ds(r, R + 8), :]
    return big[8:], pltpu.roll(big, 1, 0)[8:]


def clear_pads(nxt, prv):
    for ref in nxt:
        ref[GX : GX + 8, :] = jnp.zeros((8, GY), F32)
    for ref in prv:
        ref[0:8, :] = jnp.zeros((8, GY), F32)


def forward_step(h, u, v, column, gain, depth, p, un, vn, put):
    def first(t, r):
        here = gain * h(r)
        p[pl.ds(r, R), :] = here if column is None else here + COUP * column(r)

    over_rows(first)

    def second(t, r):
        here, after = rows_and_next(p, r)
        u0, v0 = u(r), v(r)
        un[pl.ds(r + 8, R), :] = u0 + DT * (ROT * v0 - (after - here))
        vn[pl.ds(r, R), :] = v0 - DT * (ROT * u0 + (next_lane(here) - here))

    over_rows(second)

    def third(t, r):
        u1, before = rows_and_prev(un, r)
        v1 = vn[pl.ds(r, R), :]
        put(t, r, h(r) - DT * depth * ((u1 - before) + (v1 - prev_lane(v1))), u1, v1)

    over_rows(third)


def adjoint_step(h, u, v, depth, p, un, vn, put):
    def first(t, r):
        p[pl.ds(r, R), :] = h(r)

    over_rows(first)

    def second(t, r):
        here, after = rows_and_next(p, r)
        un[pl.ds(r + 8, R), :] = u(r) + DT * depth * (after - here)
        vn[pl.ds(r, R), :] = v(r) + DT * depth * (next_lane(here) - here)

    over_rows(second)

    def third(t, r):
        u1, before = rows_and_prev(un, r)
        v1 = vn[pl.ds(r, R), :]
        put(t, r, DT * ((u1 - before) + (v1 - prev_lane(v1))), u1 - DT * ROT * v1, v1 + DT * ROT * u1)

    over_rows(third)


def laplacian_onto(column, extra, total_depth, target):
    def body(t, r):
        here, after = rows_and_next(column, r)
        dx = after - here
        start = jnp.maximum(r - 8, 0)
        edge = column[pl.ds(pl.multiple_of(start, 8), 8), :][7:8]
        rows = lax.broadcasted_iota(jnp.int32, (R, GY), 0)
        before = jnp.where(rows == 0, edge, pltpu.roll(here, 1, 0))
        back = jnp.where(rows + r > 0, here - before, 0.0)
        dy = next_lane(here) - here
        target[pl.ds(r, R), :] = extra(r) + (DT * DT * COUP * total_depth) * ((dx - back) + (dy - prev_lane(dy)))

    over_rows(body)


SCRATCH = [pltpu.VMEM((GX + 8, GY), F32), pltpu.VMEM((GX + 8, GY), F32), pltpu.VMEM((GX, GY), F32)]
STATE = pl.BlockSpec((3, 1, GX, GY), lambda k: (0, k, 0, 0))
QUARTER = GX // 4
SMEM = pl.BlockSpec(memory_space=pltpu.SMEM)


def whole(*dims):
    return pl.BlockSpec(dims, lambda k: (0,) * len(dims))


def cost(micros, moved):
    return pl.CostEstimate(flops=int(micros * 4_000_000), bytes_accessed=moved, transcendentals=0)


def params():
    return pltpu.CompilerParams(dimension_semantics=("arbitrary",), vmem_limit_bytes=67_043_328)


def add_to_half(k, t, core, mine, theirs, slot, value):
    r = pl.multiple_of((t % (CHUNKS // 2)) * R, R)

    def onto(ref):
        @pl.when(k == 0)
        def _():
            ref[slot, pl.ds(r, R), :] = value

        @pl.when(k > 0)
        def _():
            ref[slot, pl.ds(r, R), :] += value

    pl.when(t // (CHUNKS // 2) == core)(lambda: onto(mine))
    pl.when(t // (CHUNKS // 2) != core)(lambda: onto(theirs))


def put_depths(k, depth, *outs):
    @pl.when(k == 0)
    def _():
        for out in outs:
            for slot in range(2):
                out[slot, HALF:SENT, :] = jnp.full((8, GY), depth[0] + depth[1], F32)


def forward_partials_body(core, gain, depth, x, mine, theirs, p, un, vn):
    k = pl.program_id(0)
    put_depths(k, depth, mine, theirs)
    clear_pads([p], [un])

    def put(t, r, h1, u1, v1):
        add_to_half(k, t, core[0], mine, theirs, 0, x[0, 0, pl.ds(r, R), :])
        add_to_half(k, t, core[0], mine, theirs, 1, h1)

    field = lambda f: lambda r: x[f, 0, pl.ds(r, R), :]
    forward_step(field(0), field(1), field(2), None, gain[k], depth[k], p, un, vn, put)


def adjoint_partials_body(core, gain, depth, x, mine, theirs, p, un, vn, h1, u1, v1):
    k = pl.program_id(0)
    put_depths(k, depth, mine, theirs)
    clear_pads([p], [un])
    field = lambda f: lambda r: x[f, 0, pl.ds(r, R), :]
    from_ref = lambda ref: lambda r: ref[pl.ds(r, R), :]

    def put(t, r, ap, a, b):
        add_to_half(k, t, core[0], mine, theirs, 0, ap)
        h1[pl.ds(r, R), :] = x[0, 0, pl.ds(r, R), :] + gain[k] * ap
        u1[pl.ds(r, R), :] = a
        v1[pl.ds(r, R), :] = b

    adjoint_step(field(0), field(1), field(2), depth[k], p, un, vn, put)

    def put_second(t, r, ap, a, b):
        add_to_half(k, t, core[0], mine, theirs, 1, ap)

    adjoint_step(from_ref(h1), from_ref(u1), from_ref(v1), depth[k], p, un, vn, put_second)


def partials(body, core, gain, depth, state, scratch):
    halves = shape(2, SENT, GY)
    return pl.pallas_call(
        body,
        grid=(2,),
        in_specs=[SMEM, SMEM, SMEM, STATE],
        out_specs=[whole(2, SENT, GY)] * 2,
        out_shape=[halves, halves],
        scratch_shapes=scratch,
        compiler_params=params(),
        cost_estimate=cost(4, 4 << 20),
    )(core, gain, depth, state)


def join_columns(core, mine, other, total_depth, column, second):
    def first(t, r):
        s = pl.multiple_of((t % (CHUNKS // 2)) * R, R)

        @pl.when(t // (CHUNKS // 2) == core)
        def _():
            column[pl.ds(r, R), :] = mine[0, pl.ds(s, R), :]
            second[pl.ds(r, R), :] = mine[1, pl.ds(s, R), :]

        @pl.when(t // (CHUNKS // 2) != core)
        def _():
            column[pl.ds(r, R), :] = other[0, pl.ds(s, R), :]
            second[pl.ds(r, R), :] = other[1, pl.ds(s, R), :]

    clear_pads([column], [])
    over_rows(first)
    laplacian_onto(column, lambda r: second[pl.ds(r, R), :], total_depth, second)


def both_forward(x, column, second, gain, depth, p, un, vn, h1, u1, v1, put):
    field = x if callable(x) else lambda f: lambda r: x[f, 0, pl.ds(r, R), :]
    from_ref = lambda ref: lambda r: ref[pl.ds(r, R), :]

    def keep(t, r, h, u, v):
        h1[pl.ds(r, R), :] = h
        u1[pl.ds(r, R), :] = u
        v1[pl.ds(r, R), :] = v

    forward_step(field(0), field(1), field(2), from_ref(column), gain, depth, p, un, vn, keep)
    forward_step(from_ref(h1), from_ref(u1), from_ref(v1), from_ref(second), gain, depth, p, un, vn, put)


def both_adjoint(x, column, second, gain, depth, p, un, vn, h1, u1, v1, put):
    field = x if callable(x) else lambda f: lambda r: x[f, 0, pl.ds(r, R), :]
    from_ref = lambda ref: lambda r: ref[pl.ds(r, R), :]

    def keep(t, r, ap, u, v):
        h1[pl.ds(r, R), :] = field(0)(r) + gain * ap + COUP * column[pl.ds(r, R), :]
        u1[pl.ds(r, R), :] = u
        v1[pl.ds(r, R), :] = v

    def last(t, r, ap, u, v):
        put(t, r, h1[pl.ds(r, R), :] + gain * ap + COUP * second[pl.ds(r, R), :], u, v)

    adjoint_step(field(0), field(1), field(2), depth, p, un, vn, keep)
    adjoint_step(from_ref(h1), from_ref(u1), from_ref(v1), depth, p, un, vn, last)


COLUMN_SCRATCH = [pltpu.VMEM((GX + 8, GY), F32), pltpu.VMEM((GX, GY), F32)]
LEVEL_SCRATCH = [pltpu.VMEM((GX, GY), F32)] * 3
ANY = pl.BlockSpec(memory_space=pl.ANY)


def chain_terms_body(
    core, place, gain, depth, factor, x, lam, ev, mine, other, own_rows, *rest
):
    outs, (p, un, vn, h1, u1, v1, column, second, term) = rest[:LINE], rest[LINE:]
    k = pl.program_id(0)

    @pl.when(k == 0)
    def _():
        clear_pads([p], [un])
        join_columns(core[0], mine, other, mine[0, HALF : HALF + 1, :], column, second)

    def put(t, r, h, u, v):
        for f, moved in enumerate((h, u, v)):
            own = ev[f, 0, pl.ds(r, R), :] * lam[f, 0, pl.ds(r, R), :] + x[f, 0, pl.ds(r, R), :]
            own_rows[f, 0, pl.ds(r, R), :] = own
            term[f, pl.ds(r, R), :] = factor[2 * f + k] * own - moved

    both_forward(x, column, second, gain[k], depth[k], p, un, vn, h1, u1, v1, put)
    for slot, out in enumerate(outs):
        r = pl.multiple_of(lax.rem(place[0] + slot, LINE) * QUARTER, QUARTER)
        for f in range(3):
            out[0, f] = term[f, pl.ds(r, QUARTER), :]


def by_level(*dims):
    return pl.BlockSpec((1,) + dims, lambda k: (k,) + (0,) * len(dims))


PIECES = [by_level(3, QUARTER, GY)] * LINE
PIECE_SHAPES = [shape(2, 3, QUARTER, GY)] * LINE


def chain_terms(core, place, gain, depth, factor, x, lam, ev, mine, other):
    return pl.pallas_call(
        chain_terms_body,
        grid=(2,),
        in_specs=[SMEM] * 5 + [STATE] * 3 + [whole(2, SENT, GY)] * 2,
        out_specs=[STATE] + PIECES,
        out_shape=[shape(3, 2, GX, GY)] + PIECE_SHAPES,
        scratch_shapes=SCRATCH + LEVEL_SCRATCH + COLUMN_SCRATCH + [pltpu.VMEM((3, GX, GY), F32)],
        compiler_params=params(),
        cost_estimate=cost(7, 16 << 20),
        name="chain_terms",
    )(core, place, gain, depth, factor, x, lam, ev, mine, other)


def columns_of(model):
    return pl.BlockSpec((2, HALF, GY), lambda k: (model, 0, 0))


def products_body(
    core, second_way, gain, depth, depths, own, lam, xr, xr2, xv, xv2, lr, lr2, lv, lv2, fm, fo, am, ao, added,
    dual, block, p, un, vn, h1, u1, v1, fc, fs, ac, as_,
):
    k = pl.program_id(0)

    @pl.when(k == 0)
    def _():
        clear_pads([p], [un])
        join_columns(core[0], fm, fo, depths[0, 0:1, :], fc, fs)
        join_columns(core[0], am, ao, depths[0, 0:1, :], ac, as_)

    def arrived(first, second, last, second_last, flag):
        def field(f):
            a, b, i, at = (first, second, f, flag) if f < SENT_FIRST else (last, second_last, f - SENT_FIRST, flag + 1)
            return lambda r: jnp.where(second_way[at] > 0, b[i, 0, pl.ds(r, R), :], a[i, 0, pl.ds(r, R), :])

        return field

    def put(t, r, h, u, v):
        for f, moved in enumerate((h, u, v)):
            dual[f, 0, pl.ds(r, R), :] = own[f, 0, pl.ds(r, R), :] - moved

    both_forward(arrived(xr, xr2, xv, xv2, 0), fc, fs, gain[k], depth[k], p, un, vn, h1, u1, v1, put)

    def put_adjoint(t, r, h, u, v):
        block[0, 0, pl.ds(r, R), :] = (lam[0, 0, pl.ds(r, R), :] - h) + added[0, pl.ds(r, R), :]
        block[1, 0, pl.ds(r, R), :] = lam[1, 0, pl.ds(r, R), :] - u
        block[2, 0, pl.ds(r, R), :] = lam[2, 0, pl.ds(r, R), :] - v

    both_adjoint(arrived(lr, lr2, lv, lv2, 2), ac, as_, gain[k], depth[k], p, un, vn, h1, u1, v1, put_adjoint)


SENT_FIRST = 2


def fields(count):
    return pl.BlockSpec((count, 1, GX, GY), lambda k: (0, k, 0, 0))


def products(core, second_way, gain, depth, depths, own, lam, arrivals, fm, fo, am, ao, added):
    state = shape(3, 2, GX, GY)
    return pl.pallas_call(
        products_body,
        grid=(2,),
        in_specs=[SMEM] * 4
        + [pl.BlockSpec((1, 8, GY), lambda k: (0, HALF // 8, 0))]
        + [STATE] * 2
        + [fields(SENT_FIRST), fields(SENT_FIRST), fields(3 - SENT_FIRST), fields(3 - SENT_FIRST)] * 2
        + [columns_of(0), columns_of(0), columns_of(1), columns_of(1)]
        + [pl.BlockSpec((1, GX, GY), lambda k: (k, 0, 0))],
        out_specs=[STATE] * 2,
        out_shape=[state, state],
        scratch_shapes=SCRATCH + LEVEL_SCRATCH + COLUMN_SCRATCH * 2,
        compiler_params=params(),
        cost_estimate=cost(12, 24 << 20),
        name="products",
    )(core, second_way, gain, depth, depths, own, lam, *arrivals, fm, fo, am, ao, added)


SUB = QUARTER // LINE
PACKED = 3 * SUB + 8
PARTS = [by_level(PACKED, GY)] * LINE
CARRIES = by_level(3 * SUB, GY)


def in_place_order(place, pieces, ordered):
    for slot, piece in enumerate(pieces):
        ordered[lax.rem(place[0] + slot, LINE)] = piece[0]


def factor_after(place, slots, level, f, j):
    slot = lax.rem(j - place[0] + LINE, LINE)
    values = [ref[2 * f + level] for ref in slots]
    return jnp.where(slot < 2, jnp.where(slot == 0, values[0], values[1]), jnp.where(slot == 2, values[2], values[3]))


def line_total_body(place, line, d0, d1, d2, d3, a0, a1, a2, a3, *rest):
    outs, ordered = rest[:LINE], rest[LINE]
    level = pl.program_id(0)
    in_place_order(place, (a0, a1, a2, a3), ordered)
    rows = lax.broadcasted_iota(jnp.int32, (8, GY), 0)
    plane = jnp.zeros((8, GY), F32)
    for f in range(3):
        factors = [factor_after(place, (d0, d1, d2, d3), level, f, j) for j in range(LINE)]
        plane = jnp.where(rows == f, (factors[0] * factors[1]) * (factors[2] * factors[3]), plane)
        for slot, out in enumerate(outs):
            r = pl.multiple_of(lax.rem(line[0] + slot, LINE) * SUB, SUB)
            value = ordered[0, f, pl.ds(r, SUB), :]
            for j in range(1, LINE):
                value = factors[j] * value + ordered[j, f, pl.ds(r, SUB), :]
            out[0, SUB * f : SUB * f + SUB, :] = value
    for out in outs:
        out[0, 3 * SUB :, :] = plane


ORDERED = pltpu.VMEM((LINE, 3, QUARTER, GY), F32)


def line_total(place, line, factors, pieces):
    return pl.pallas_call(
        line_total_body,
        grid=(2,),
        in_specs=[SMEM] * (2 + LINE) + PIECES,
        out_specs=PARTS,
        out_shape=[shape(2, PACKED, GY)] * LINE,
        scratch_shapes=[ORDERED],
        compiler_params=params(),
        cost_estimate=cost(1, 2 << 20),
        name="line_total",
    )(place, line, *factors, *pieces)


def lines_onward(carry, ordered, f):
    out = [carry]
    for j in range(LINE):
        factor = ordered[j, 3 * SUB + f : 3 * SUB + f + 1, :]
        out.append(factor * out[-1] + ordered[j, SUB * f : SUB * f + SUB, :])
    return out


def put_in_order(line, parts, ordered):
    for slot, part in enumerate(parts):
        ordered[lax.rem(line[0] + slot, LINE)] = part[0]


def half_total_body(line, a0, a1, a2, a3, out, ordered):
    put_in_order(line, (a0, a1, a2, a3), ordered)
    for f in range(3):
        out[0, SUB * f : SUB * f + SUB, :] = lines_onward(jnp.zeros((SUB, GY), F32), ordered, f)[LINE]


def half_total(line, parts):
    return pl.pallas_call(
        half_total_body,
        grid=(2,),
        in_specs=[SMEM] + PARTS,
        out_specs=CARRIES,
        out_shape=shape(2, 3 * SUB, GY),
        scratch_shapes=[pltpu.VMEM((LINE, PACKED, GY), F32)],
        compiler_params=params(),
        cost_estimate=cost(1, 1 << 20),
        name="half_total",
    )(line, *parts)


def line_carries_body(line, carried, a0, a1, a2, a3, o0, o1, o2, o3, ordered, carries):
    put_in_order(line, (a0, a1, a2, a3), ordered)
    for f in range(3):
        rows = slice(SUB * f, SUB * f + SUB)
        for j, value in enumerate(lines_onward(carried[0, rows, :], ordered, f)[:LINE]):
            carries[j, rows, :] = value
    for slot, out in enumerate((o0, o1, o2, o3)):
        out[0] = carries[lax.rem(line[0] + slot, LINE)]


def line_carries(line, carried, parts):
    return pl.pallas_call(
        line_carries_body,
        grid=(2,),
        in_specs=[SMEM, CARRIES] + PARTS,
        out_specs=[CARRIES] * LINE,
        out_shape=[shape(2, 3 * SUB, GY)] * LINE,
        scratch_shapes=[pltpu.VMEM((LINE, PACKED, GY), F32), pltpu.VMEM((LINE, 3 * SUB, GY), F32)],
        compiler_params=params(),
        cost_estimate=cost(1, 1 << 20),
        name="line_carries",
    )(line, carried, *parts)


def spread_body(place, line, d0, d1, d2, d3, c0, c1, c2, c3, a0, a1, a2, a3, o0, o1, o2, o3, ordered):
    level = pl.program_id(0)
    in_place_order(place, (a0, a1, a2, a3), ordered)
    for f in range(3):
        factors = [factor_after(place, (d0, d1, d2, d3), level, f, j) for j in range(LINE)]
        for part, carried in enumerate((c0, c1, c2, c3)):
            r = pl.multiple_of(lax.rem(line[0] + part, LINE) * SUB, SUB)
            value = carried[0, SUB * f : SUB * f + SUB, :]
            for j in range(LINE):
                term = ordered[j, f, pl.ds(r, SUB), :]
                ordered[j, f, pl.ds(r, SUB), :] = value
                value = factors[j] * value + term
    for slot, out in enumerate((o0, o1, o2, o3)):
        out[0] = ordered[lax.rem(place[0] + slot, LINE)]


def spread(place, line, factors, carried, pieces):
    return pl.pallas_call(
        spread_body,
        grid=(2,),
        in_specs=[SMEM] * (2 + LINE) + [CARRIES] * LINE + PIECES,
        out_specs=PIECES,
        out_shape=PIECE_SHAPES,
        scratch_shapes=[ORDERED],
        compiler_params=params(),
        cost_estimate=cost(1, 4 << 20),
        name="spread",
    )(place, line, *factors, *carried, *pieces)


def finish_body(place, own, a0, a1, a2, a3, out):
    for slot, part in enumerate((a0, a1, a2, a3)):
        rows = pl.ds(pl.multiple_of(lax.rem(place[0] + slot, LINE) * QUARTER, QUARTER), QUARTER)
        for f in range(3):
            out[f, 0, rows, :] = own[f, 0, rows, :] + part[0, f]


def finish(place, own, parts):
    return pl.pallas_call(
        finish_body,
        grid=(2,),
        in_specs=[SMEM, STATE] + PIECES,
        out_specs=STATE,
        out_shape=shape(3, 2, GX, GY),
        compiler_params=params(),
        cost_estimate=cost(5, 9 << 20),
        name="finish",
    )(place, own, *parts)


def along(axis, distance):
    size = lax.axis_size(axis)
    return [(i, i + distance) for i in range(size) if 0 <= i + distance < size]


def swap(array, bit):
    return lax.ppermute(array, "lev", [(i, i ^ bit) for i in range(lax.axis_size("lev"))])


def around(array, distance):
    size = lax.axis_size("tm")
    return lax.ppermute(
        array, "tm", [(i, i - i % LINE + (i % LINE + distance) % LINE) for i in range(size)]
    )


def sideways(array, distance):
    size, four = lax.axis_size("tm"), LINE * LINE
    return lax.ppermute(
        array, "tm", [(i, i - i % four + (i % four + LINE * distance) % four) for i in range(size)]
    )


def to_second_half(array):
    half = lax.axis_size("tm") // 2
    return lax.ppermute(array, "tm", [(i, i + half) for i in range(half)])


def shards(
    increment, multiplier, error_var, obs_cell, obs_dual, obs_var, level_gain, mean_depth, chain_decay
):
    x, lam, ev = increment[0], multiplier[0], error_var[0]
    lev = lax.axis_index("lev")
    core, ylo = lev % 2, lev // 2
    core_arr = core.astype(jnp.int32).reshape(1)
    slab = lax.axis_index("tm")
    place = (slab % LINE).astype(jnp.int32).reshape(1)

    def exchanged(pieces, move=around):
        out = [pieces[0]]
        for slot, distance in ((3, -1), (2, 2), (1, 1)):
            out.append(move(pieces[slot], distance))
        return out

    own = lax.ppermute(chain_decay[0].reshape(6), "tm", along("tm", -1))
    size = lax.axis_size("tm")
    mid, half_ring = size // 2, lambda d: [(i, i - i % mid + (i % mid + d) % mid) for i in range(size)]
    arrivals = []
    for array, step in ((x, 1), (lam, -1)):
        ends = (0, mid) if step > 0 else (mid - 1, size - 1)
        first = lax.ppermute(array[:SENT_FIRST], "tm", half_ring(step))
        first_2 = lax.ppermute(first, "tm", [ends if step > 0 else ends[::-1]])
        last = around(array[SENT_FIRST:], step)
        hops = [(i, i + LINE * step) for i in range(0 if step > 0 else LINE - 1, size, LINE)]
        last_2 = lax.ppermute(last, "tm", [(i, j) for i, j in hops if 0 <= j < size])
        arrivals += [first, first_2, last, last_2]
    second_way = jnp.stack(
        [slab % mid == 0, slab % LINE == 0, slab % mid == mid - 1, slab % LINE == LINE - 1]
    ).astype(jnp.int32)
    here = exchanged([own] * LINE)
    fm, ft = partials(forward_partials_body, core_arr, level_gain, mean_depth, x, SCRATCH)
    fm = fm + swap(ft, 1)
    fm = fm + swap(fm, 2)
    fo = swap(fm, 1)
    am, at = partials(adjoint_partials_body, core_arr, level_gain, mean_depth, lam, SCRATCH + LEVEL_SCRATCH)
    am = am + swap(at, 1)
    am = am + swap(am, 2)

    own_rows, *terms = chain_terms(
        core_arr, place, level_gain, mean_depth, own, x, lam, ev, fm, fo
    )
    cells, duals, terms[0] = lax.optimization_barrier((obs_cell[0], obs_dual[0], terms[0]))
    rows, cols = cells // GY, cells % GY
    level = lax.broadcasted_iota(jnp.int32, rows.shape, 0)
    seen = []
    for k in range(2):
        seen.append(x[jnp.zeros_like(rows[k]), jnp.full_like(rows[k], k), rows[k], cols[k]])
    obs_product = obs_var[0] * duals + jnp.stack(seen)
    added = jnp.zeros(x[0].shape, F32).at[level, rows, cols].add(duals)

    line = (slab // LINE % LINE).astype(jnp.int32).reshape(1)
    pieces = exchanged(terms)
    pieces[0], added = lax.optimization_barrier((pieces[0], added))
    sums = line_total(place, line, here, pieces)
    sums = exchanged(sums, sideways)
    carried = to_second_half(half_total(line, sums))
    carries = line_carries(line, carried, sums)
    carries = exchanged(carries, sideways)
    parts = spread(place, line, here, carries, pieces)
    parts = exchanged(parts)
    chain = finish(place, own_rows, parts)

    quarter = HALF // 2
    fq = lax.ppermute(
        lax.dynamic_slice_in_dim(fm, ylo * quarter, quarter, 1), "tm", along("tm", 1)
    )
    aq = lax.ppermute(lax.dynamic_slice_in_dim(am, ylo * quarter, quarter, 1), "tm", along("tm", -1))
    q = jnp.concatenate([fq, aq])
    qo = swap(q, 2)
    half = jnp.where(ylo == 0, jnp.concatenate([q, qo], 1), jnp.concatenate([qo, q], 1))
    other = swap(half, 1)

    dual, block = products(
        core_arr, second_way, level_gain, mean_depth, fm, own_rows, lam, arrivals,
        half, other, half, other, added,
    )
    return dual[None], obs_product[None], block[None], chain[None]


def solution(mesh):
    state = P("tm", None, "lev", None, None)
    obs = P("tm", "lev", None)

    return jax.shard_map(
        shards,
        mesh=mesh,
        in_specs=(state, state, state, obs, obs, obs, P("lev"), P("lev"), P("tm", None, "lev")),
        out_specs=(state, obs, state, state),
        check_vma=False,
    )
```
